32 devices in a mesh: dp: 1 (over z), inner: 4 (over y), vocab: 8 (over x, core).
Axes of the slice: x: 4, y: 4, z: 1, core: 2. Of those that a mesh axis runs over, the one named last changes fastest.
The devices are a block of a 4x4x8 slice.
Arguments:
- hidden: bfloat16 [256, 2304], P('dp')
- w_head: bfloat16 [2304, 256000], P(None, ('vocab', 'inner'))
- inv_temp: float32 [256], P('dp')
- target_id: int32 [256], P('dp')
Outputs:
- output 1: float32 [256, 256000], P('dp', ('vocab', 'inner'))
- output 2: float32 [256], P('dp')
All inputs are finite; a program needn't handle non-finite values.
Results may differ from the reference program's by a relative error of at most 0.001.
Values are sent between devices in bfloat16 or wider.
A program may use at most 768 MiB of HBM per device.

```python
import jax
import jax.numpy as jnp

B = 256
D = 2304
V = 256000


def setup_inputs(seed: int = 0, part: int = 0) -> dict:
    base_key = jax.random.key(seed)
    rows_key, weight_key = jax.random.split(base_key)
    part_key = jax.random.fold_in(rows_key, part)
    noise_key, shift_key, slope_key, temp_key, target_key = jax.random.split(part_key, 5)
    dim_even = (jnp.arange(D) % 2) == 0
    shift_amp = jax.random.uniform(shift_key, (B, 1), jnp.float32, 0.0, 2.0)
    slope_amp = jax.random.uniform(slope_key, (B, 1), jnp.float32, 0.8, 1.2)
    row_mean = jnp.where(dim_even[None, :], shift_amp, slope_amp)
    hidden = jax.random.normal(noise_key, (B, D), jnp.float32) + row_mean
    inv_temp = jax.random.uniform(temp_key, (B,), jnp.float32, 0.6, 1.4)
    token_rank = jnp.log1p(jnp.arange(V).astype(jnp.float32))
    col_mean = jnp.where(dim_even[:, None], 50.0, -token_rank[None, :]) * (2.0 / D)
    w_head = jax.random.normal(weight_key, (D, V), jnp.float32) * (D ** -0.5) + col_mean
    low_key, high_key = jax.random.split(target_key)
    any_id = jax.random.randint(low_key, (B,), 0, V)
    late_id = jax.random.randint(high_key, (B,), V // 2, V)
    target_id = jnp.where(jnp.arange(B) % 4 == 0, any_id, late_id).astype(jnp.int32)
    return {'hidden': hidden.astype(jnp.bfloat16), 'w_head': w_head.astype(jnp.bfloat16), 'inv_temp': inv_temp, 'target_id': target_id}


def reference(hidden, w_head, inv_temp, target_id):
    logits = jnp.dot(hidden, w_head, preferred_element_type=jnp.float32) * inv_temp[:, None]
    row_max = jnp.max(logits, axis=1, keepdims=True)
    exp_shift = jnp.exp(logits - row_max)
    row_sum = jnp.sum(exp_shift, axis=1, keepdims=True)
    cdf_table = jnp.cumsum(exp_shift / row_sum, axis=1)
    col_ids = jnp.arange(V)
    cdf_target = jnp.sum(jnp.where(col_ids[None, :] == target_id[:, None], cdf_table, 0.0), axis=1)
    return cdf_table, cdf_target
```

```python
import functools

import jax
import jax.numpy as jnp
from jax import lax
from jax.experimental import pallas as pl
from jax.experimental.pallas import tpu as pltpu
from jax.sharding import PartitionSpec as P

VOCAB_AXES = ('vocab', 'inner')
MESH = pl.DeviceIdType.MESH
LANES = 128
SUB = 8
TILE = 800


def stream_kernel(n_vocab, n_inner, h_hbm, w_hbm, inv_hbm, tgt_hbm,
                  c_ref, scale_ref, off_ref, ct_ref,
                  h_v, wbuf, inv_v, tgt_v, zbuf, z_top, m_tile, s_tile, t_tile,
                  stats, in_sem, w_sem, send_sem, recv_sem):
    peers = n_vocab * n_inner
    rows = h_v.shape[0]
    width = w_hbm.shape[0]
    halves = rows // LANES
    tiles = width // TILE
    run = TILE // SUB
    me = lax.axis_index('vocab') * n_inner + lax.axis_index('inner')

    def tokens(t):
        return pl.ds(pl.multiple_of(t * TILE, TILE), TILE)

    def w_copy(t):
        return pltpu.make_async_copy(w_hbm.at[tokens(t), :], wbuf.at[tokens(t), :], w_sem.at[t])

    small = [pltpu.make_async_copy(h_hbm, h_v, in_sem.at[0]),
             pltpu.make_async_copy(inv_hbm, inv_v, in_sem.at[1]),
             pltpu.make_async_copy(tgt_hbm, tgt_v, in_sem.at[2])]
    for copy in small:
        copy.start()

    @pl.loop(0, tiles)
    def _(t):
        w_copy(t).start()

    def peer(k):
        p = lax.rem(me + k, peers)
        return {'vocab': p // n_inner, 'inner': lax.rem(p, n_inner)}

    barrier = pltpu.get_barrier_semaphore()

    @pl.loop(1, peers)
    def _(k):
        pl.semaphore_signal(barrier, inc=1, device_id=peer(k), device_id_type=MESH)

    for copy in small:
        copy.wait()
    sub = lax.broadcasted_iota(jnp.int32, (SUB, LANES), 0)

    def logits(t):
        slot = lax.rem(t, 2)
        z = lax.dot_general(wbuf[tokens(t), :], h_v[...], (((1,), (1,)), ((), ())),
                            preferred_element_type=jnp.float32)
        for i in range(halves):
            zi = z[:, i * LANES:(i + 1) * LANES] * inv_v[pl.ds(i, 1), :]
            zbuf[slot, i] = zi
            z_top[slot, i] = jnp.max(zi.reshape(run, SUB, LANES), axis=0)

    def weigh(t):
        slot = lax.rem(t, 2)
        for i in range(halves):
            top = jnp.broadcast_to(jnp.max(z_top[slot, i], axis=0, keepdims=True), (SUB, LANES))
            goal = tgt_v[pl.ds(i, 1), :] - (me * width + t * TILE) - sub * run
            goal = jnp.minimum(goal, run - 1)
            total = jnp.zeros((SUB, LANES), jnp.float32)
            upto = jnp.zeros((SUB, LANES), jnp.float32)
            for j in range(run):
                total = total + jnp.exp(zbuf[slot, i, pl.ds(j, SUB, stride=run), :] - top)
                c_ref[i, pl.ds(pl.multiple_of(t * TILE + j * SUB, SUB), SUB), :] = total
                upto = jnp.where(goal == j, total, upto)
            m_tile[t, i] = top
            s_tile[t, i] = total
            t_tile[t, i] = upto

    w_copy(0).wait()
    logits(0)

    @pl.loop(1, tiles)
    def _(t):
        w_copy(t).wait()
        logits(t)
        weigh(t - 1)

    weigh(tiles - 1)

    mix = jnp.zeros((SUB, LANES), jnp.float32)
    for i in range(halves):
        m = m_tile[0, i]
        for t in range(1, tiles):
            m = jnp.maximum(m, m_tile[t, i])
        s = jnp.zeros((SUB, LANES), jnp.float32)
        u = jnp.zeros((SUB, LANES), jnp.float32)
        for t in range(tiles):
            f = jnp.exp(m_tile[t, i] - m)
            s = s + s_tile[t, i] * f
            u = u + t_tile[t, i] * f
        mix = jnp.where((sub == 4 * i) | (sub == 4 * i + 1), m, mix)
        mix = jnp.where(sub == 4 * i + 2, jnp.sum(s, axis=0, keepdims=True), mix)
        mix = jnp.where(sub == 4 * i + 3, jnp.sum(u, axis=0, keepdims=True), mix)
    stats[me] = mix

    pl.semaphore_wait(barrier, peers - 1)

    @pl.loop(1, peers)
    def _(k):
        pltpu.make_async_remote_copy(
            src_ref=stats.at[me], dst_ref=stats.at[me], send_sem=send_sem, recv_sem=recv_sem,
            device_id=peer(k), device_id_type=MESH).start()

    everyone = stats.at[pl.ds(0, peers - 1)]
    done = pltpu.make_async_remote_copy(
        src_ref=everyone, dst_ref=everyone, send_sem=send_sem, recv_sem=recv_sem,
        device_id=peer(0), device_id_type=MESH)
    done.wait_recv()

    peak = stats[0]
    for p in range(1, peers):
        peak = jnp.maximum(peak, stats[p])
    whole = jnp.zeros((SUB, LANES), jnp.float32)
    before = jnp.zeros((SUB, LANES), jnp.float32)
    for p in range(peers):
        part = pltpu.roll(jnp.exp(stats[p] - peak), 2, 0) * stats[p]
        whole = whole + part
        before = before + jnp.where(p < me, part, 0.0)
    offset = before / whole
    reached = whole / pltpu.roll(whole, 1, 0)
    for i in range(halves):
        def row(x, k):
            return jnp.broadcast_to(x[4 * i + k:4 * i + k + 1, :], (SUB, LANES))
        ct_ref[pl.ds(i, 1), :] = reached[4 * i + 3:4 * i + 4, :]
        m, s, base = row(peak, 0), row(whole, 2), row(offset, 2)
        for t in range(tiles):
            scale = jnp.exp(m_tile[t, i] - m) / s
            scale_ref[t, i] = scale
            mass = s_tile[t, i] * scale
            ahead = mass
            for d in (1, 2, 4):
                ahead = ahead + jnp.where(sub >= d, pltpu.roll(ahead, d, 0), 0.0)
            off_ref[t, i] = base + jnp.where(sub >= 1, pltpu.roll(ahead, 1, 0), 0.0)
            base = base + jnp.broadcast_to(ahead[SUB - 1:SUB, :], (SUB, LANES))
    done.wait_send()


def finish_kernel(c_ref, scale_ref, off_ref, ct_ref, out_hbm, ct_out, stage, sem):
    halves, width = c_ref.shape[:2]
    tiles = width // TILE
    run = TILE // SUB
    ct_out[...] = ct_ref[...]

    def copy(t, i):
        here = pl.ds(pl.multiple_of(t * TILE, TILE), TILE)
        return pltpu.make_async_copy(stage.at[i, here, :], out_hbm.at[here, pl.ds(i * LANES, LANES)], sem.at[i])

    @pl.loop(0, tiles)
    def _(t):
        for i in range(halves):
            scale, offset = scale_ref[t, i], off_ref[t, i]
            for j in range(run):
                v = c_ref[i, pl.ds(pl.multiple_of(t * TILE + j * SUB, SUB), SUB), :]
                stage[i, pl.ds(t * TILE + j, SUB, stride=run), :] = v * scale + offset
            copy(t, i).start()

    for i in range(halves):
        pltpu.make_async_copy(stage.at[i], out_hbm.at[:, pl.ds(i * LANES, LANES)], sem.at[i]).wait()


def solution(mesh):
    n_vocab, n_inner = mesh.shape['vocab'], mesh.shape['inner']
    peers = n_vocab * n_inner

    def local_step(hidden, w_shard, inv_temp, target_id):
        rows, depth = hidden.shape
        width = w_shard.shape[1]
        tiles = width // TILE
        halves = rows // LANES
        f32, bf16 = jnp.float32, jnp.bfloat16
        hbm = pl.BlockSpec(memory_space=pl.ANY)
        vmem = pl.BlockSpec(memory_space=pltpu.VMEM)
        c, scale, offset, ct = pl.pallas_call(
            functools.partial(stream_kernel, n_vocab, n_inner),
            out_shape=[pltpu.VMEM((halves, width, LANES), f32), pltpu.VMEM((tiles, halves, SUB, LANES), f32),
                       pltpu.VMEM((tiles, halves, SUB, LANES), f32), pltpu.VMEM((halves, LANES), f32)],
            in_specs=[hbm] * 4,
            out_specs=[vmem] * 4,
            scratch_shapes=[
                pltpu.VMEM((rows, depth), bf16),
                pltpu.VMEM((width, depth), bf16),
                pltpu.VMEM((halves, LANES), f32),
                pltpu.VMEM((halves, LANES), jnp.int32),
                pltpu.VMEM((2, halves, TILE, LANES), f32),
                pltpu.VMEM((2, halves, SUB, LANES), f32),
                pltpu.VMEM((tiles, halves, SUB, LANES), f32),
                pltpu.VMEM((tiles, halves, SUB, LANES), f32),
                pltpu.VMEM((tiles, halves, SUB, LANES), f32),
                pltpu.VMEM((peers, SUB, LANES), f32),
                pltpu.SemaphoreType.DMA((3,)),
                pltpu.SemaphoreType.DMA((tiles,)),
                pltpu.SemaphoreType.DMA,
                pltpu.SemaphoreType.DMA,
            ],
            compiler_params=pltpu.CompilerParams(
                collective_id=0, has_side_effects=True, vmem_limit_bytes=52 * 2**20),
        )(hidden, w_shard.T, inv_temp.reshape(halves, LANES), target_id.reshape(halves, LANES))
        table, target = pl.pallas_call(
            finish_kernel,
            out_shape=[pltpu.HBM((width, rows), f32), pltpu.HBM((halves, LANES), f32)],
            in_specs=[vmem] * 4,
            out_specs=[pl.BlockSpec(memory_space=pltpu.HBM), vmem],
            scratch_shapes=[pltpu.VMEM((halves, width, LANES), f32), pltpu.SemaphoreType.DMA((halves,))],
            compiler_params=pltpu.CompilerParams(vmem_limit_bytes=20 * 2**20),
        )(c, scale, offset, ct)
        return table.T, target.reshape(rows)

    return jax.shard_map(local_step, mesh=mesh, in_specs=(P('dp', None), P(None, VOCAB_AXES), P('dp'), P('dp')), out_specs=(P('dp', VOCAB_AXES), P('dp')), check_vma=False)
```

```python
import functools

import jax
import jax.numpy as jnp
from jax import lax
from jax.experimental import pallas as pl
from jax.experimental.pallas import tpu as pltpu
from jax.sharding import PartitionSpec as P

VOCAB_AXES = ('vocab', 'inner')
MESH = pl.DeviceIdType.MESH
LANES = 128
SUB = 8
HEAD, BODY, TAIL = (320, 480), 800, (480, 320)


def plan(width):
    count = (width - sum(HEAD) - sum(TAIL)) // BODY
    sizes = list(HEAD) + [BODY] * count + list(TAIL)
    assert sum(sizes) == width
    starts = [sum(sizes[:i]) for i in range(len(sizes))]
    return list(zip(starts, sizes)), len(HEAD), count


def hint(x, k):
    return x if isinstance(x, int) else pl.multiple_of(x, k)


def above(x, sub):
    total = x
    for d in (1, 2, 4):
        total = total + jnp.where(sub >= d, pltpu.roll(total, d, 0), 0.0)
    return total - x, jnp.broadcast_to(total[SUB - 1:SUB, :], (SUB, LANES))


def stream_kernel(n_vocab, n_inner, h_hbm, w_hbm, inv_hbm, tgt_hbm,
                  c_ref, scale_ref, start_ref, ends_ref, ct_ref,
                  h_v, wbuf, inv_v, tgt_v, zbuf, ebuf, z_top, m_tile, s_tile, t_tile,
                  stats, in_sem, w_sem, send_sem, recv_sem):
    peers = n_vocab * n_inner
    rows = h_v.shape[0]
    width = w_hbm.shape[0]
    halves = rows // LANES
    tiles, heads, count = plan(width)
    my_vocab, my_inner = lax.axis_index('vocab'), lax.axis_index('inner')
    me = my_vocab * n_inner + my_inner
    sub = lax.broadcasted_iota(jnp.int32, (SUB, LANES), 0)

    def w_copy(t, start, size):
        here = pl.ds(hint(start, 16), size)
        return pltpu.make_async_copy(w_hbm.at[here, :], wbuf.at[here, :], w_sem.at[t])

    small = [pltpu.make_async_copy(h_hbm, h_v, in_sem.at[0]),
             pltpu.make_async_copy(inv_hbm, inv_v, in_sem.at[1]),
             pltpu.make_async_copy(tgt_hbm, tgt_v, in_sem.at[2])]
    for copy in small:
        copy.start()
    for t, (start, size) in enumerate(tiles):
        w_copy(t, start, size).start()

    far = sorted(((dv, di) for dv in range(n_vocab) for di in range(n_inner) if dv or di),
                 key=lambda o: -(min(o[0], n_vocab - o[0]) / 2 + min(o[1], n_inner - o[1])))

    def peer(dv, di):
        return {'vocab': lax.rem(my_vocab + dv, n_vocab), 'inner': lax.rem(my_inner + di, n_inner)}

    barrier = pltpu.get_barrier_semaphore()
    for offset in far:
        pl.semaphore_signal(barrier, inc=1, device_id=peer(*offset), device_id_type=MESH)

    for copy in small:
        copy.wait()

    def logits(start, size):
        z = lax.dot_general(wbuf[pl.ds(hint(start, 16), size), :], h_v[...], (((1,), (1,)), ((), ())),
                            preferred_element_type=jnp.float32)
        for i in range(halves):
            zi = z[:, i * LANES:(i + 1) * LANES] * inv_v[pl.ds(i, 1), :]
            zbuf[i, pl.ds(0, size), :] = zi
            z_top[i] = jnp.max(zi.reshape(size // SUB, SUB, LANES), axis=0)

    def weigh(t, start, size):
        run = size // SUB
        for i in range(halves):
            top = jnp.broadcast_to(jnp.max(z_top[i], axis=0, keepdims=True), (SUB, LANES))
            total = jnp.zeros((SUB, LANES), jnp.float32)
            for j in range(run):
                e = jnp.exp(zbuf[i, pl.ds(j, SUB, stride=run), :] - top)
                ebuf[i, pl.ds(j * SUB, SUB), :] = e
                total = total + e
            running, total = above(total, sub)
            goal = tgt_v[pl.ds(i, 1), :] - (me * width + start)
            upto = jnp.where((goal >= size) & (sub == 0), total, 0.0)
            goal = goal - sub * run
            for j in range(run):
                running = running + ebuf[i, pl.ds(j * SUB, SUB), :]
                c_ref[i, pl.ds(start + j, SUB, stride=run), :] = running
                upto = jnp.where(goal == j, running, upto)
            m_tile[t, i] = top
            s_tile[t, i] = total
            t_tile[t, i] = upto

    def step(t, start, size, before=None):
        w_copy(t, start, size).wait()
        if before is not None:
            weigh(t - 1, *before)
        logits(start, size)

    for t in range(heads + 1):
        step(t, *tiles[t], tiles[t - 1] if t else None)

    @pl.loop(heads + 1, heads + count)
    def _(t):
        start = tiles[heads][0] + (t - heads) * BODY
        step(t, start, BODY, (start - BODY, BODY))

    for t in range(heads + count, len(tiles)):
        step(t, *tiles[t], tiles[t - 1])
    weigh(len(tiles) - 1, *tiles[-1])

    mix = jnp.zeros((SUB, LANES), jnp.float32)
    for i in range(halves):
        m = m_tile[0, i]
        for t in range(1, len(tiles)):
            m = jnp.maximum(m, m_tile[t, i])
        s = jnp.zeros((SUB, LANES), jnp.float32)
        u = jnp.zeros((SUB, LANES), jnp.float32)
        for t in range(len(tiles)):
            f = jnp.exp(m_tile[t, i] - m)
            scale_ref[t, i] = f
            start_ref[t, i] = s
            s = s + s_tile[t, i] * f
            u = u + t_tile[t, i] * f
        mix = jnp.where((sub == 4 * i) | (sub == 4 * i + 1), m, mix)
        mix = jnp.where(sub == 4 * i + 2, s, mix)
        mix = jnp.where(sub == 4 * i + 3, jnp.sum(u, axis=0, keepdims=True), mix)
    stats[me] = mix

    pl.semaphore_wait(barrier, peers - 1)
    for offset in far:
        pltpu.make_async_remote_copy(
            src_ref=stats.at[me], dst_ref=stats.at[me], send_sem=send_sem, recv_sem=recv_sem,
            device_id=peer(*offset), device_id_type=MESH).start()

    everyone = stats.at[pl.ds(0, peers - 1)]
    done = pltpu.make_async_remote_copy(
        src_ref=everyone, dst_ref=everyone, send_sem=send_sem, recv_sem=recv_sem,
        device_id=peer(0, 0), device_id_type=MESH)
    done.wait_recv()

    peak = stats[0]
    for p in range(1, peers):
        peak = jnp.maximum(peak, stats[p])
    whole = jnp.zeros((SUB, LANES), jnp.float32)
    before = jnp.zeros((SUB, LANES), jnp.float32)
    for p in range(peers):
        part = pltpu.roll(jnp.exp(stats[p] - peak), 2, 0) * stats[p]
        whole = whole + part
        before = before + jnp.where(p < me, part, 0.0)
    factor = pltpu.roll(jnp.exp(stats[me] - peak), 2, 0) / whole
    offset = before / whole
    reached = whole / pltpu.roll(whole, 1, 0)
    for i in range(halves):
        ct_ref[pl.ds(i, 1), :] = reached[4 * i + 3:4 * i + 4, :]
        ends_ref[0, i] = jnp.broadcast_to(factor[4 * i + 2:4 * i + 3, :], (SUB, LANES))
        ends_ref[1, i] = jnp.broadcast_to(offset[4 * i + 2:4 * i + 3, :], (SUB, LANES))
    done.wait_send()


def finish_kernel(c_ref, scale_ref, start_ref, ends_ref, ct_ref, out_hbm, ct_out, stage, sem):
    halves, width = c_ref.shape[:2]
    tiles, heads, count = plan(width)
    ct_out[...] = ct_ref[...]

    def emit(t, start, size):
        first = start // SUB
        scale = [scale_ref[t, i] * ends_ref[0, i] for i in range(halves)]
        offset = [start_ref[t, i] * ends_ref[0, i] + ends_ref[1, i] for i in range(halves)]
        for k in range(size // SUB):
            for i in range(halves):
                v = c_ref[i, pl.ds(hint(start + k * SUB, SUB), SUB), :]
                stage[first + k, i] = v * scale[i] + offset[i]
        here = pl.ds(first, size // SUB)
        pltpu.make_async_copy(stage.at[here], out_hbm.at[here], sem).start()

    for t in range(heads):
        emit(t, *tiles[t])

    @pl.loop(heads, heads + count)
    def _(t):
        emit(t, tiles[heads][0] + (t - heads) * BODY, BODY)

    for t in range(heads + count, len(tiles)):
        emit(t, *tiles[t])

    pltpu.make_async_copy(stage, out_hbm, sem).wait()


def solution(mesh):
    n_vocab, n_inner = mesh.shape['vocab'], mesh.shape['inner']
    peers = n_vocab * n_inner
    f32, bf16 = jnp.float32, jnp.bfloat16
    hbm = pl.BlockSpec(memory_space=pl.ANY)
    vmem = pl.BlockSpec(memory_space=pltpu.VMEM)

    def local_step(hidden, w_shard, inv_temp, target_id):
        rows, depth = hidden.shape
        width = w_shard.shape[1]
        halves = rows // LANES
        tiles = len(plan(width)[0])
        small = (tiles, halves, SUB, LANES)
        packed = (width // SUB, halves, SUB, LANES)
        parts = pl.pallas_call(
            functools.partial(stream_kernel, n_vocab, n_inner),
            name='stream',
            out_shape=[pltpu.VMEM((halves, width, LANES), f32), pltpu.VMEM(small, f32), pltpu.VMEM(small, f32),
                       pltpu.VMEM((2, halves, SUB, LANES), f32), pltpu.VMEM((halves, LANES), f32)],
            in_specs=[hbm] * 4,
            out_specs=[vmem] * 5,
            scratch_shapes=[
                pltpu.VMEM((rows, depth), bf16),
                pltpu.VMEM((width, depth), bf16),
                pltpu.VMEM((halves, LANES), f32),
                pltpu.VMEM((halves, LANES), jnp.int32),
                pltpu.VMEM((halves, BODY, LANES), f32),
                pltpu.VMEM((halves, BODY, LANES), f32),
                pltpu.VMEM((halves, SUB, LANES), f32),
                pltpu.VMEM(small, f32),
                pltpu.VMEM(small, f32),
                pltpu.VMEM(small, f32),
                pltpu.VMEM((peers, SUB, LANES), f32),
                pltpu.SemaphoreType.DMA((3,)),
                pltpu.SemaphoreType.DMA((tiles,)),
                pltpu.SemaphoreType.DMA,
                pltpu.SemaphoreType.DMA,
            ],
            compiler_params=pltpu.CompilerParams(
                collective_id=0, has_side_effects=True, vmem_limit_bytes=52 * 2**20),
        )(hidden, w_shard.T, inv_temp.reshape(halves, LANES), target_id.reshape(halves, LANES))
        table, target = pl.pallas_call(
            finish_kernel,
            name='finish',
            out_shape=[pltpu.HBM(packed, f32), pltpu.HBM((halves, LANES), f32)],
            in_specs=[vmem] * 5,
            out_specs=[pl.BlockSpec(memory_space=pltpu.HBM), vmem],
            scratch_shapes=[pltpu.VMEM(packed, f32), pltpu.SemaphoreType.DMA],
            compiler_params=pltpu.CompilerParams(vmem_limit_bytes=20 * 2**20),
        )(*parts)
        return table.transpose(0, 2, 1, 3).reshape(width, rows).T, target.reshape(rows)

    return jax.shard_map(local_step, mesh=mesh, in_specs=(P('dp', None), P(None, VOCAB_AXES), P('dp'), P('dp')), out_specs=(P('dp', VOCAB_AXES), P('dp')), check_vma=False)
```

```python
import functools

import jax
import jax.numpy as jnp
from jax import lax
from jax.experimental import pallas as pl
from jax.experimental.pallas import tpu as pltpu
from jax.sharding import PartitionSpec as P

VOCAB_AXES = ('vocab', 'inner')
MESH = pl.DeviceIdType.MESH
LANES = 128
SUB = 8
BODY = 800
WIDE = 256
BLOCKS = 25


def hint(x, k):
    return x if isinstance(x, int) else pl.multiple_of(x, k)


def above(x, sub):
    total = x
    for d in (1, 2, 4):
        total = total + jnp.where(sub >= d, pltpu.roll(total, d, 0), 0.0)
    return total - x, jnp.broadcast_to(total[SUB - 1:SUB, :], (SUB, LANES))


def stream_kernel(h_hbm, w_hbm, inv_hbm, tgt_hbm,
                  c_ref, scale_ref, start_ref, mix_ref,
                  h_v, wbuf, inv_v, tgt_v, zbuf, ebuf, m_tile, s_tile, t_tile, in_sem, w_sem):
    rows, depth = h_v.shape
    width = w_hbm.shape[0]
    halves = rows // LANES
    count = width // BODY
    part = BODY // 2
    run = BODY // SUB
    me = lax.axis_index('vocab') * lax.axis_size('inner') + lax.axis_index('inner')
    sub = lax.broadcasted_iota(jnp.int32, (SUB, LANES), 0)

    def w_copy(t):
        here = pl.ds(hint(t * BODY, 16), BODY)
        return pltpu.make_async_copy(w_hbm.at[here, :], wbuf.at[here, :], w_sem.at[t])

    small = [pltpu.make_async_copy(h_hbm, h_v, in_sem.at[0]),
             pltpu.make_async_copy(inv_hbm, inv_v, in_sem.at[1]),
             pltpu.make_async_copy(tgt_hbm, tgt_v, in_sem.at[2])]
    for copy in small:
        copy.start()

    @pl.loop(0, count)
    def _(t):
        w_copy(t).start()

    for copy in small:
        copy.wait()

    def weigh(t, tops):
        start = t * BODY
        for i in range(halves):
            top = jnp.broadcast_to(jnp.max(tops[i], axis=0, keepdims=True), (SUB, LANES))
            sums = [jnp.zeros((SUB, LANES), jnp.float32)] * 4
            for j in range(run):
                e = jnp.exp(zbuf[i, pl.ds(j, SUB, stride=run), :] - top)
                ebuf[i, pl.ds(j * SUB, SUB), :] = e
                sums[j % 4] = sums[j % 4] + e
            running, total = above((sums[0] + sums[1]) + (sums[2] + sums[3]), sub)
            goal = tgt_v[pl.ds(i, 1), :] - (me * width + start)
            upto = jnp.where((goal >= BODY) & (sub == 0), total, 0.0)
            goal = goal - sub * run
            for j in range(run):
                running = running + ebuf[i, pl.ds(j * SUB, SUB), :]
                c_ref[i, pl.ds(start + j, SUB, stride=run), :] = running
                upto = jnp.where(goal == j, running, upto)
            m_tile[t, i] = top
            s_tile[t, i] = total
            t_tile[t, i] = upto

    def multiply(*accs):
        accs = (accs[:2], accs[2:])

        def push(k):
            for q in range(2):
                pltpu.matmul_push_rhs(h_v[:, pl.ds(k * WIDE, WIDE)], 0, q, transpose=True)

        def drain(t, slot):
            tops = [None] * halves
            for q in range(2):
                z = pltpu.matmul_pop(accs[q][slot])
                for i in range(halves):
                    zi = z[:, i * LANES:(i + 1) * LANES] * inv_v[pl.ds(i, 1), :]
                    zbuf[i, pl.ds(q * part, part), :] = zi
                    top = jnp.max(zi.reshape(part // SUB, SUB, LANES), axis=0)
                    tops[i] = top if q == 0 else jnp.maximum(tops[i], top)
            weigh(t, tops)

        def step(t, slot, first=False, final=False):
            w_copy(t).wait()
            for k in range(depth // WIDE):
                for q in range(2):
                    pltpu.matmul_acc_lhs(
                        accs[q][slot], wbuf[pl.ds(hint(t * BODY + q * part, 16), part), pl.ds(k * WIDE, WIDE)],
                        load_staged_rhs=0)
                if k < depth // WIDE - 1:
                    push(k + 1)
                elif not final:
                    push(0)
                if k == 1 and not first:
                    drain(t - 1, 1 - slot)

        for q in range(2):
            for slot in range(2):
                pltpu.matmul_pop(accs[q][slot])
        push(0)
        step(0, 0, first=True)
        step(1, 1)

        @pl.loop(1, count // 2 - 1)
        def _(p):
            step(2 * p, 0)
            step(2 * p + 1, 1)

        step(count - 2, 0)
        step(count - 1, 1, final=True)
        drain(count - 1, 1)

    pl.run_scoped(multiply, *[pltpu.ACC(q)((part, rows), jnp.float32) for q in (0, 0, 1, 1)])

    mix = jnp.zeros((SUB, LANES), jnp.float32)
    for i in range(halves):
        m = m_tile[0, i]
        for t in range(1, count):
            m = jnp.maximum(m, m_tile[t, i])
        s = jnp.zeros((SUB, LANES), jnp.float32)
        u = jnp.zeros((SUB, LANES), jnp.float32)
        for t in range(count):
            f = jnp.exp(m_tile[t, i] - m)
            scale_ref[t, i] = f
            start_ref[t, i] = s
            s = s + s_tile[t, i] * f
            u = u + t_tile[t, i] * f
        mix = jnp.where((sub == 4 * i) | (sub == 4 * i + 1), m, mix)
        mix = jnp.where(sub == 4 * i + 2, s, mix)
        mix = jnp.where(sub == 4 * i + 3, jnp.sum(u, axis=0, keepdims=True), mix)
    mix_ref[...] = mix


def exchange_kernel(n_vocab, n_inner, mix_ref, ends_ref, ct_ref, stats, send_sem, recv_sem):
    peers = n_vocab * n_inner
    halves = ct_ref.shape[0]
    my_vocab, my_inner = lax.axis_index('vocab'), lax.axis_index('inner')
    me = my_vocab * n_inner + my_inner

    far = sorted(((dv, di) for dv in range(n_vocab) for di in range(n_inner) if dv or di),
                 key=lambda o: -(min(o[0], n_vocab - o[0]) / 2 + min(o[1], n_inner - o[1])))

    def peer(dv, di):
        return {'vocab': lax.rem(my_vocab + dv, n_vocab), 'inner': lax.rem(my_inner + di, n_inner)}

    stats[me] = mix_ref[...]
    barrier = pltpu.get_barrier_semaphore()
    for offset in far:
        pl.semaphore_signal(barrier, inc=1, device_id=peer(*offset), device_id_type=MESH)
    pl.semaphore_wait(barrier, peers - 1)
    for offset in far:
        pltpu.make_async_remote_copy(
            src_ref=stats.at[me], dst_ref=stats.at[me], send_sem=send_sem, recv_sem=recv_sem,
            device_id=peer(*offset), device_id_type=MESH).start()

    everyone = stats.at[pl.ds(0, peers - 1)]
    done = pltpu.make_async_remote_copy(
        src_ref=everyone, dst_ref=everyone, send_sem=send_sem, recv_sem=recv_sem,
        device_id=peer(0, 0), device_id_type=MESH)
    done.wait_recv()

    peak = stats[0]
    for p in range(1, peers):
        peak = jnp.maximum(peak, stats[p])
    whole = jnp.zeros((SUB, LANES), jnp.float32)
    before = jnp.zeros((SUB, LANES), jnp.float32)
    for p in range(peers):
        mass = pltpu.roll(jnp.exp(stats[p] - peak), 2, 0) * stats[p]
        whole = whole + mass
        before = before + jnp.where(p < me, mass, 0.0)
    factor = pltpu.roll(jnp.exp(stats[me] - peak), 2, 0) / whole
    offset = before / whole
    reached = whole / pltpu.roll(whole, 1, 0)
    for i in range(halves):
        ct_ref[pl.ds(i, 1), :] = reached[4 * i + 3:4 * i + 4, :]
        ends_ref[0, i] = jnp.broadcast_to(factor[4 * i + 2:4 * i + 3, :], (SUB, LANES))
        ends_ref[1, i] = jnp.broadcast_to(offset[4 * i + 2:4 * i + 3, :], (SUB, LANES))
    done.wait_send()


def finish_kernel(c_ref, scale_ref, start_ref, ends_ref, ct_ref, out_hbm, ct_out, stage, sem):
    halves, width = c_ref.shape[:2]
    parts = BODY // SUB // BLOCKS
    ct_out[...] = ct_ref[...]

    @pl.loop(0, width // SUB // BLOCKS)
    def _(b):
        t = b // parts
        scale = [scale_ref[t, i] * ends_ref[0, i] for i in range(halves)]
        offset = [start_ref[t, i] * ends_ref[0, i] + ends_ref[1, i] for i in range(halves)]
        first = b * BLOCKS
        for k in range(BLOCKS):
            for i in range(halves):
                v = c_ref[i, pl.ds(hint((first + k) * SUB, SUB), SUB), :]
                stage[first + k, i] = v * scale[i] + offset[i]
        here = pl.ds(first, BLOCKS)
        pltpu.make_async_copy(stage.at[here], out_hbm.at[here], sem).start()

    pltpu.make_async_copy(stage, out_hbm, sem).wait()


def solution(mesh):
    n_vocab, n_inner = mesh.shape['vocab'], mesh.shape['inner']
    peers = n_vocab * n_inner
    f32, bf16 = jnp.float32, jnp.bfloat16
    hbm = pl.BlockSpec(memory_space=pl.ANY)
    vmem = pl.BlockSpec(memory_space=pltpu.VMEM)

    def local_step(hidden, w_shard, inv_temp, target_id):
        rows, depth = hidden.shape
        width = w_shard.shape[1]
        halves = rows // LANES
        tiles = width // BODY
        small = (tiles, halves, SUB, LANES)
        packed = (width // SUB, halves, SUB, LANES)
        c, scale, start, mix = pl.pallas_call(
            stream_kernel,
            name='stream',
            out_shape=[pltpu.VMEM((halves, width, LANES), f32), pltpu.VMEM(small, f32), pltpu.VMEM(small, f32),
                       pltpu.VMEM((SUB, LANES), f32)],
            in_specs=[hbm] * 4,
            out_specs=[vmem] * 4,
            scratch_shapes=[
                pltpu.VMEM((rows, depth), bf16),
                pltpu.VMEM((width, depth), bf16),
                pltpu.VMEM((halves, LANES), f32),
                pltpu.VMEM((halves, LANES), jnp.int32),
                pltpu.VMEM((halves, BODY, LANES), f32),
                pltpu.VMEM((halves, BODY, LANES), f32),
                pltpu.VMEM(small, f32),
                pltpu.VMEM(small, f32),
                pltpu.VMEM(small, f32),
                pltpu.SemaphoreType.DMA((3,)),
                pltpu.SemaphoreType.DMA((tiles,)),
            ],
            compiler_params=pltpu.CompilerParams(vmem_limit_bytes=52 * 2**20),
        )(hidden, w_shard.T, inv_temp.reshape(halves, LANES), target_id.reshape(halves, LANES))
        ends, ct = pl.pallas_call(
            functools.partial(exchange_kernel, n_vocab, n_inner),
            name='exchange',
            out_shape=[pltpu.VMEM((2, halves, SUB, LANES), f32), pltpu.VMEM((halves, LANES), f32)],
            in_specs=[vmem],
            out_specs=[vmem] * 2,
            scratch_shapes=[pltpu.VMEM((peers, SUB, LANES), f32), pltpu.SemaphoreType.DMA, pltpu.SemaphoreType.DMA],
            compiler_params=pltpu.CompilerParams(collective_id=0, has_side_effects=True, vmem_limit_bytes=2**20),
        )(mix)
        table, target = pl.pallas_call(
            finish_kernel,
            name='finish',
            out_shape=[pltpu.HBM(packed, f32), pltpu.HBM((halves, LANES), f32)],
            in_specs=[vmem] * 5,
            out_specs=[pl.BlockSpec(memory_space=pltpu.HBM), vmem],
            scratch_shapes=[pltpu.VMEM(packed, f32), pltpu.SemaphoreType.DMA],
            compiler_params=pltpu.CompilerParams(vmem_limit_bytes=20 * 2**20),
        )(c, scale, start, ends, ct)
        return table.transpose(0, 2, 1, 3).reshape(width, rows).T, target.reshape(rows)

    return jax.shard_map(local_step, mesh=mesh, in_specs=(P('dp', None), P(None, VOCAB_AXES), P('dp'), P('dp')), out_specs=(P('dp', VOCAB_AXES), P('dp')), check_vma=False)
```

```python
import functools

import jax
import jax.numpy as jnp
from jax import lax
from jax.experimental import pallas as pl
from jax.experimental.pallas import tpu as pltpu
from jax.sharding import PartitionSpec as P

VOCAB_AXES = ('vocab', 'inner')
MESH = pl.DeviceIdType.MESH
LANES = 128
SUB = 8
BODY = 800
WIDE = 256
BLOCKS = 25


def hint(x, k):
    return x if isinstance(x, int) else pl.multiple_of(x, k)


def above(x, sub):
    total = x
    for d in (1, 2, 4):
        total = total + jnp.where(sub >= d, pltpu.roll(total, d, 0), 0.0)
    return total - x, jnp.broadcast_to(total[SUB - 1:SUB, :], (SUB, LANES))


def stream_kernel(h_hbm, w_hbm, inv_hbm, tgt_hbm,
                  c_ref, scale_ref, start_ref, mix_ref,
                  h_v, wbuf, inv_v, tgt_v, zbuf, ebuf, m_tile, s_tile, t_tile, in_sem, w_sem):
    rows, depth = h_v.shape
    width = w_hbm.shape[0]
    halves = rows // LANES
    count = width // BODY
    part = BODY // 2
    run = BODY // SUB
    me = lax.axis_index('vocab') * lax.axis_size('inner') + lax.axis_index('inner')
    sub = lax.broadcasted_iota(jnp.int32, (SUB, LANES), 0)

    def w_copy(t):
        here = pl.ds(hint(t * BODY, 16), BODY)
        return pltpu.make_async_copy(w_hbm.at[here, :], wbuf.at[here, :], w_sem.at[t])

    small = [pltpu.make_async_copy(h_hbm, h_v, in_sem.at[0]),
             pltpu.make_async_copy(inv_hbm, inv_v, in_sem.at[1]),
             pltpu.make_async_copy(tgt_hbm, tgt_v, in_sem.at[2])]
    for copy in small:
        copy.start()

    @pl.loop(0, count)
    def _(t):
        w_copy(t).start()

    for copy in small:
        copy.wait()

    def weigh(t, tops):
        start = t * BODY
        for i in range(halves):
            top = jnp.broadcast_to(jnp.max(tops[i], axis=0, keepdims=True), (SUB, LANES))
            sums = [jnp.zeros((SUB, LANES), jnp.float32)] * 4
            for j in range(run):
                e = jnp.exp(zbuf[i, pl.ds(j, SUB, stride=run), :] - top)
                ebuf[i, pl.ds(j * SUB, SUB), :] = e
                sums[j % 4] = sums[j % 4] + e
            running, total = above((sums[0] + sums[1]) + (sums[2] + sums[3]), sub)
            goal = tgt_v[pl.ds(i, 1), :] - (me * width + start)
            upto = jnp.where((goal >= BODY) & (sub == 0), total, 0.0)
            goal = goal - sub * run
            for j in range(run):
                running = running + ebuf[i, pl.ds(j * SUB, SUB), :]
                c_ref[i, pl.ds(start + j, SUB, stride=run), :] = running
                upto = jnp.where(goal == j, running, upto)
            m_tile[t, i] = top
            s_tile[t, i] = total
            t_tile[t, i] = upto

    def multiply(*accs):
        accs = (accs[:2], accs[2:])

        def push(k):
            for q in range(2):
                pltpu.matmul_push_rhs(h_v[:, pl.ds(k * WIDE, WIDE)], 0, q, transpose=True)

        def drain(t, slot):
            tops = [None] * halves
            for q in range(2):
                z = pltpu.matmul_pop(accs[q][slot])
                for i in range(halves):
                    zi = z[:, i * LANES:(i + 1) * LANES] * inv_v[pl.ds(i, 1), :]
                    zbuf[i, pl.ds(q * part, part), :] = zi
                    top = jnp.max(zi.reshape(part // SUB, SUB, LANES), axis=0)
                    tops[i] = top if q == 0 else jnp.maximum(tops[i], top)
            weigh(t, tops)

        def step(t, slot, first=False, final=False):
            w_copy(t).wait()
            for k in range(depth // WIDE):
                for q in range(2):
                    pltpu.matmul_acc_lhs(
                        accs[q][slot], wbuf[pl.ds(hint(t * BODY + q * part, 16), part), pl.ds(k * WIDE, WIDE)],
                        load_staged_rhs=0)
                if k < depth // WIDE - 1:
                    push(k + 1)
                elif not final:
                    push(0)
                if k == 1 and not first:
                    drain(t - 1, 1 - slot)

        for q in range(2):
            for slot in range(2):
                pltpu.matmul_pop(accs[q][slot])
        push(0)
        step(0, 0, first=True)
        step(1, 1)

        @pl.loop(1, count // 2 - 1)
        def _(p):
            step(2 * p, 0)
            step(2 * p + 1, 1)

        step(count - 2, 0)
        step(count - 1, 1, final=True)
        drain(count - 1, 1)

    pl.run_scoped(multiply, *[pltpu.ACC(q)((part, rows), jnp.float32) for q in (0, 0, 1, 1)])

    mix = jnp.zeros((SUB, LANES), jnp.float32)
    for i in range(halves):
        m = m_tile[0, i]
        for t in range(1, count):
            m = jnp.maximum(m, m_tile[t, i])
        s = jnp.zeros((SUB, LANES), jnp.float32)
        u = jnp.zeros((SUB, LANES), jnp.float32)
        for t in range(count):
            f = jnp.exp(m_tile[t, i] - m)
            scale_ref[t, i] = f
            start_ref[t, i] = s
            s = s + s_tile[t, i] * f
            u = u + t_tile[t, i] * f
        mix = jnp.where((sub == 4 * i) | (sub == 4 * i + 1), m, mix)
        mix = jnp.where(sub == 4 * i + 2, s, mix)
        mix = jnp.where(sub == 4 * i + 3, jnp.sum(u, axis=0, keepdims=True), mix)
    mix_ref[...] = mix


def exchange_kernel(n_vocab, n_inner, mix_ref, ends_ref, ct_ref, stats, send_sem, recv_sem):
    peers = n_vocab * n_inner
    halves = ct_ref.shape[0]
    my_vocab, my_inner = lax.axis_index('vocab'), lax.axis_index('inner')
    me = my_vocab * n_inner + my_inner

    far = sorted(((dv, di) for dv in range(n_vocab) for di in range(n_inner) if dv or di),
                 key=lambda o: -(min(o[0], n_vocab - o[0]) / 2 + min(o[1], n_inner - o[1])))

    def peer(dv, di):
        return {'vocab': lax.rem(my_vocab + dv, n_vocab), 'inner': lax.rem(my_inner + di, n_inner)}

    stats[me] = mix_ref[...]
    barrier = pltpu.get_barrier_semaphore()
    for offset in far:
        pl.semaphore_signal(barrier, inc=1, device_id=peer(*offset), device_id_type=MESH)
    pl.semaphore_wait(barrier, peers - 1)
    for offset in far:
        pltpu.make_async_remote_copy(
            src_ref=stats.at[me], dst_ref=stats.at[me], send_sem=send_sem, recv_sem=recv_sem,
            device_id=peer(*offset), device_id_type=MESH).start()

    everyone = stats.at[pl.ds(0, peers - 1)]
    done = pltpu.make_async_remote_copy(
        src_ref=everyone, dst_ref=everyone, send_sem=send_sem, recv_sem=recv_sem,
        device_id=peer(0, 0), device_id_type=MESH)
    done.wait_recv()

    peak = stats[0]
    for p in range(1, peers):
        peak = jnp.maximum(peak, stats[p])
    whole = jnp.zeros((SUB, LANES), jnp.float32)
    before = jnp.zeros((SUB, LANES), jnp.float32)
    for p in range(peers):
        mass = pltpu.roll(jnp.exp(stats[p] - peak), 2, 0) * stats[p]
        whole = whole + mass
        before = before + jnp.where(p < me, mass, 0.0)
    factor = pltpu.roll(jnp.exp(stats[me] - peak), 2, 0) / whole
    offset = before / whole
    reached = whole / pltpu.roll(whole, 1, 0)
    for i in range(halves):
        ct_ref[pl.ds(i, 1), :] = reached[4 * i + 3:4 * i + 4, :]
        ends_ref[0, i] = jnp.broadcast_to(factor[4 * i + 2:4 * i + 3, :], (SUB, LANES))
        ends_ref[1, i] = jnp.broadcast_to(offset[4 * i + 2:4 * i + 3, :], (SUB, LANES))
    done.wait_send()


def finish_kernel(c_ref, scale_ref, start_ref, ends_ref, ct_ref, out_hbm, ct_out, stage, sem):
    halves, width = c_ref.shape[:2]
    parts = BODY // SUB // BLOCKS
    target = pltpu.make_async_copy(ct_ref, ct_out, sem.at[1])
    target.start()

    @pl.loop(0, width // SUB // BLOCKS)
    def _(b):
        t = b // parts
        scale = [scale_ref[t, i] * ends_ref[0, i] for i in range(halves)]
        offset = [start_ref[t, i] * ends_ref[0, i] + ends_ref[1, i] for i in range(halves)]
        first = b * BLOCKS
        for k in range(BLOCKS):
            for i in range(halves):
                v = c_ref[i, pl.ds(hint((first + k) * SUB, SUB), SUB), :]
                stage[first + k, i] = v * scale[i] + offset[i]
        here = pl.ds(first, BLOCKS)
        pltpu.make_async_copy(stage.at[here], out_hbm.at[here], sem.at[0]).start()

    pltpu.make_async_copy(stage, out_hbm, sem.at[0]).wait()
    target.wait()


def solution(mesh):
    n_vocab, n_inner = mesh.shape['vocab'], mesh.shape['inner']
    peers = n_vocab * n_inner
    f32, bf16 = jnp.float32, jnp.bfloat16
    hbm = pl.BlockSpec(memory_space=pl.ANY)
    vmem = pl.BlockSpec(memory_space=pltpu.VMEM)

    def local_step(hidden, w_shard, inv_temp, target_id):
        rows, depth = hidden.shape
        width = w_shard.shape[1]
        halves = rows // LANES
        tiles = width // BODY
        small = (tiles, halves, SUB, LANES)
        packed = (width // SUB, halves, SUB, LANES)
        c, scale, start, mix = pl.pallas_call(
            stream_kernel,
            name='stream',
            out_shape=[pltpu.VMEM((halves, width, LANES), f32), pltpu.VMEM(small, f32), pltpu.VMEM(small, f32),
                       pltpu.VMEM((SUB, LANES), f32)],
            in_specs=[hbm] * 4,
            out_specs=[vmem] * 4,
            scratch_shapes=[
                pltpu.VMEM((rows, depth), bf16),
                pltpu.VMEM((width, depth), bf16),
                pltpu.VMEM((halves, LANES), f32),
                pltpu.VMEM((halves, LANES), jnp.int32),
                pltpu.VMEM((halves, BODY, LANES), f32),
                pltpu.VMEM((halves, BODY, LANES), f32),
                pltpu.VMEM(small, f32),
                pltpu.VMEM(small, f32),
                pltpu.VMEM(small, f32),
                pltpu.SemaphoreType.DMA((3,)),
                pltpu.SemaphoreType.DMA((tiles,)),
            ],
            compiler_params=pltpu.CompilerParams(vmem_limit_bytes=52 * 2**20),
        )(hidden, w_shard.T, inv_temp.reshape(halves, LANES), target_id.reshape(halves, LANES))
        ends, ct = pl.pallas_call(
            functools.partial(exchange_kernel, n_vocab, n_inner),
            name='exchange',
            out_shape=[pltpu.VMEM((2, halves, SUB, LANES), f32), pltpu.VMEM((halves, LANES), f32)],
            in_specs=[vmem],
            out_specs=[vmem] * 2,
            scratch_shapes=[pltpu.VMEM((peers, SUB, LANES), f32), pltpu.SemaphoreType.DMA, pltpu.SemaphoreType.DMA],
            compiler_params=pltpu.CompilerParams(collective_id=0, has_side_effects=True, vmem_limit_bytes=2**20),
        )(mix)
        table, target = pl.pallas_call(
            finish_kernel,
            name='finish',
            out_shape=[pltpu.HBM(packed, f32), pltpu.HBM((halves, LANES), f32)],
            in_specs=[vmem] * 5,
            out_specs=[pl.BlockSpec(memory_space=pltpu.HBM)] * 2,
            scratch_shapes=[pltpu.VMEM(packed, f32), pltpu.SemaphoreType.DMA((2,))],
            compiler_params=pltpu.CompilerParams(vmem_limit_bytes=20 * 2**20),
        )(c, scale, start, ends, ct)
        return table.transpose(0, 2, 1, 3).reshape(width, rows).T, target.reshape(rows)

    return jax.shard_map(local_step, mesh=mesh, in_specs=(P('dp', None), P(None, VOCAB_AXES), P('dp'), P('dp')), out_specs=(P('dp', VOCAB_AXES), P('dp')), check_vma=False)
```

```python
import functools

import jax
import jax.numpy as jnp
from jax import lax
from jax.experimental import pallas as pl
from jax.experimental.pallas import tpu as pltpu
from jax.sharding import PartitionSpec as P

VOCAB_AXES = ('vocab', 'inner')
MESH = pl.DeviceIdType.MESH
LANES = 128
SUB = 8
BODY = 800
WIDE = 256
BLOCKS = 25


def hint(x, k):
    return x if isinstance(x, int) else pl.multiple_of(x, k)


def above(x, sub):
    total = x
    for d in (1, 2, 4):
        total = total + jnp.where(sub >= d, pltpu.roll(total, d, 0), 0.0)
    return total - x, jnp.broadcast_to(total[SUB - 1:SUB, :], (SUB, LANES))


def weigh(start, tops, tgt_v, zbuf, ebuf, c_ref, first):
    halves = len(tops)
    run = BODY // SUB
    sub = lax.broadcasted_iota(jnp.int32, (SUB, LANES), 0)
    out = []
    for i in range(halves):
        top = jnp.broadcast_to(jnp.max(tops[i], axis=0, keepdims=True), (SUB, LANES))
        sums = [jnp.zeros((SUB, LANES), jnp.float32)] * 4
        for j in range(run):
            e = jnp.exp(zbuf[i, pl.ds(j, SUB, stride=run), :] - top)
            ebuf[i, pl.ds(j * SUB, SUB), :] = e
            sums[j % 4] = sums[j % 4] + e
        running, total = above((sums[0] + sums[1]) + (sums[2] + sums[3]), sub)
        goal = tgt_v[pl.ds(i, 1), :] - start
        upto = jnp.where((goal >= BODY) & (sub == 0), total, 0.0)
        goal = goal - sub * run
        for j in range(run):
            running = running + ebuf[i, pl.ds(j * SUB, SUB), :]
            c_ref[i, pl.ds(first + j, SUB, stride=run), :] = running
            upto = jnp.where(goal == j, running, upto)
        out.append((top, total, upto))
    return out


def stream_kernel(h_hbm, w_hbm, inv_hbm, tgt_hbm,
                  c_ref, zbuf, top_ref, m_tile, s_tile, t_tile, tgt_v,
                  h_v, wbuf, inv_v, ebuf, in_sem, w_sem):
    rows, depth = h_v.shape
    width = w_hbm.shape[0]
    halves = rows // LANES
    count = width // BODY
    part = BODY // 2
    run = BODY // SUB
    me = lax.axis_index('vocab') * lax.axis_size('inner') + lax.axis_index('inner')
    sub = lax.broadcasted_iota(jnp.int32, (SUB, LANES), 0)

    def w_copy(t):
        here = pl.ds(hint(t * BODY, 16), BODY)
        return pltpu.make_async_copy(w_hbm.at[here, :], wbuf.at[here, :], w_sem.at[t])

    small = [pltpu.make_async_copy(h_hbm, h_v, in_sem.at[0]),
             pltpu.make_async_copy(inv_hbm, inv_v, in_sem.at[1]),
             pltpu.make_async_copy(tgt_hbm, tgt_v, in_sem.at[2])]
    for copy in small:
        copy.start()

    @pl.loop(0, count)
    def _(t):
        w_copy(t).start()

    for copy in small:
        copy.wait()

    def multiply(*accs):
        accs = (accs[:2], accs[2:])

        def push(k):
            for q in range(2):
                pltpu.matmul_push_rhs(h_v[:, pl.ds(k * WIDE, WIDE)], 0, q, transpose=True)

        def drain(t, slot):
            tops = [None] * halves
            for q in range(2):
                z = pltpu.matmul_pop(accs[q][slot])
                for i in range(halves):
                    zi = z[:, i * LANES:(i + 1) * LANES] * inv_v[pl.ds(i, 1), :]
                    zbuf[i, pl.ds(q * part, part), :] = zi
                    top = jnp.max(zi.reshape(part // SUB, SUB, LANES), axis=0)
                    tops[i] = top if q == 0 else jnp.maximum(tops[i], top)
            return tops

        def step(t, slot, first=False, final=False):
            w_copy(t).wait()
            for k in range(depth // WIDE):
                for q in range(2):
                    pltpu.matmul_acc_lhs(
                        accs[q][slot], wbuf[pl.ds(hint(t * BODY + q * part, 16), part), pl.ds(k * WIDE, WIDE)],
                        load_staged_rhs=0)
                if k < depth // WIDE - 1:
                    push(k + 1)
                elif not final:
                    push(0)
                if k == 1 and not first:
                    tops = drain(t - 1, 1 - slot)
                    start = (t - 1) * BODY
                    for i, (m, s, u) in enumerate(weigh(me * width + start, tops, tgt_v, zbuf, ebuf, c_ref, start)):
                        m_tile[t - 1, i] = m
                        s_tile[t - 1, i] = s
                        t_tile[t - 1, i] = u

        for q in range(2):
            for slot in range(2):
                pltpu.matmul_pop(accs[q][slot])
        push(0)
        step(0, 0, first=True)
        step(1, 1)

        @pl.loop(1, count // 2 - 1)
        def _(p):
            step(2 * p, 0)
            step(2 * p + 1, 1)

        step(count - 2, 0)
        step(count - 1, 1, final=True)
        for i, top in enumerate(drain(count - 1, 1)):
            top_ref[i] = top

    pl.run_scoped(multiply, *[pltpu.ACC(q)((part, rows), jnp.float32) for q in (0, 0, 1, 1)])


def exchange_kernel(n_vocab, n_inner, zbuf, top_ref, m_tile, s_tile, t_tile, tgt_v,
                    c_last, scale_ref, start_ref, ends_ref, ct_ref, ebuf, stats, send_sem, recv_sem):
    peers = n_vocab * n_inner
    halves = ct_ref.shape[0]
    my_vocab, my_inner = lax.axis_index('vocab'), lax.axis_index('inner')
    me = my_vocab * n_inner + my_inner

    far = sorted(((dv, di) for dv in range(n_vocab) for di in range(n_inner) if dv or di),
                 key=lambda o: -(min(o[0], n_vocab - o[0]) / 2 + min(o[1], n_inner - o[1])))

    def peer(dv, di):
        return {'vocab': lax.rem(my_vocab + dv, n_vocab), 'inner': lax.rem(my_inner + di, n_inner)}

    barrier = pltpu.get_barrier_semaphore()
    for offset in far:
        pl.semaphore_signal(barrier, inc=1, device_id=peer(*offset), device_id_type=MESH)

    count = m_tile.shape[0] + 1
    last = (count - 1) * BODY
    final = weigh(me * (count * BODY) + last, [top_ref[i] for i in range(halves)], tgt_v, zbuf, ebuf, c_last, 0)
    sub = lax.broadcasted_iota(jnp.int32, (SUB, LANES), 0)
    mix = jnp.zeros((SUB, LANES), jnp.float32)
    for i in range(halves):
        known = [(m_tile[t, i], s_tile[t, i], t_tile[t, i]) for t in range(count - 1)] + [final[i]]
        m = functools.reduce(jnp.maximum, [k[0] for k in known])
        s = jnp.zeros((SUB, LANES), jnp.float32)
        u = jnp.zeros((SUB, LANES), jnp.float32)
        for t in range(count):
            f = jnp.exp(known[t][0] - m)
            scale_ref[t, i] = f
            start_ref[t, i] = s
            s = s + known[t][1] * f
            u = u + known[t][2] * f
        mix = jnp.where((sub == 4 * i) | (sub == 4 * i + 1), m, mix)
        mix = jnp.where(sub == 4 * i + 2, s, mix)
        mix = jnp.where(sub == 4 * i + 3, jnp.sum(u, axis=0, keepdims=True), mix)
    stats[me] = mix
    pl.semaphore_wait(barrier, peers - 1)
    for offset in far:
        pltpu.make_async_remote_copy(
            src_ref=stats.at[me], dst_ref=stats.at[me], send_sem=send_sem, recv_sem=recv_sem,
            device_id=peer(*offset), device_id_type=MESH).start()

    everyone = stats.at[pl.ds(0, peers - 1)]
    done = pltpu.make_async_remote_copy(
        src_ref=everyone, dst_ref=everyone, send_sem=send_sem, recv_sem=recv_sem,
        device_id=peer(0, 0), device_id_type=MESH)
    done.wait_recv()

    peak = stats[0]
    for p in range(1, peers):
        peak = jnp.maximum(peak, stats[p])
    whole = jnp.zeros((SUB, LANES), jnp.float32)
    before = jnp.zeros((SUB, LANES), jnp.float32)
    for p in range(peers):
        mass = pltpu.roll(jnp.exp(stats[p] - peak), 2, 0) * stats[p]
        whole = whole + mass
        before = before + jnp.where(p < me, mass, 0.0)
    factor = pltpu.roll(jnp.exp(stats[me] - peak), 2, 0) / whole
    offset = before / whole
    reached = whole / pltpu.roll(whole, 1, 0)
    for i in range(halves):
        ct_ref[pl.ds(i, 1), :] = reached[4 * i + 3:4 * i + 4, :]
        ends_ref[0, i] = jnp.broadcast_to(factor[4 * i + 2:4 * i + 3, :], (SUB, LANES))
        ends_ref[1, i] = jnp.broadcast_to(offset[4 * i + 2:4 * i + 3, :], (SUB, LANES))
    done.wait_send()


def finish_kernel(c_ref, c_last, scale_ref, start_ref, ends_ref, ct_ref, out_hbm, ct_out, stage, sem):
    halves = c_ref.shape[0]
    parts = BODY // SUB // BLOCKS
    early = c_ref.shape[1] // SUB // BLOCKS
    target = pltpu.make_async_copy(ct_ref, ct_out, sem.at[1])
    target.start()

    def emit(b, source, origin):
        t = b // parts
        scale = [scale_ref[t, i] * ends_ref[0, i] for i in range(halves)]
        offset = [start_ref[t, i] * ends_ref[0, i] + ends_ref[1, i] for i in range(halves)]
        first = b * BLOCKS
        for k in range(BLOCKS):
            for i in range(halves):
                v = source[i, pl.ds(hint((first - origin + k) * SUB, SUB), SUB), :]
                stage[first + k, i] = v * scale[i] + offset[i]
        here = pl.ds(first, BLOCKS)
        pltpu.make_async_copy(stage.at[here], out_hbm.at[here], sem.at[0]).start()

    @pl.loop(0, early)
    def _(b):
        emit(b, c_ref, 0)

    @pl.loop(early, early + parts)
    def _(b):
        emit(b, c_last, early * BLOCKS)

    pltpu.make_async_copy(stage, out_hbm, sem.at[0]).wait()
    target.wait()


def solution(mesh):
    n_vocab, n_inner = mesh.shape['vocab'], mesh.shape['inner']
    peers = n_vocab * n_inner
    f32, bf16 = jnp.float32, jnp.bfloat16
    hbm = pl.BlockSpec(memory_space=pl.ANY)
    vmem = pl.BlockSpec(memory_space=pltpu.VMEM)

    def local_step(hidden, w_shard, inv_temp, target_id):
        rows, depth = hidden.shape
        width = w_shard.shape[1]
        halves = rows // LANES
        tiles = width // BODY
        small, early = (tiles, halves, SUB, LANES), (tiles - 1, halves, SUB, LANES)
        block = (halves, BODY, LANES)
        packed = (width // SUB, halves, SUB, LANES)
        c, *state = pl.pallas_call(
            stream_kernel,
            name='stream',
            out_shape=[pltpu.VMEM((halves, width - BODY, LANES), f32), pltpu.VMEM(block, f32),
                       pltpu.VMEM((halves, SUB, LANES), f32), pltpu.VMEM(early, f32), pltpu.VMEM(early, f32),
                       pltpu.VMEM(early, f32), pltpu.VMEM((halves, LANES), jnp.int32)],
            in_specs=[hbm] * 4,
            out_specs=[vmem] * 7,
            scratch_shapes=[
                pltpu.VMEM((rows, depth), bf16),
                pltpu.VMEM((width, depth), bf16),
                pltpu.VMEM((halves, LANES), f32),
                pltpu.VMEM(block, f32),
                pltpu.SemaphoreType.DMA((3,)),
                pltpu.SemaphoreType.DMA((tiles,)),
            ],
            compiler_params=pltpu.CompilerParams(vmem_limit_bytes=50 * 2**20),
        )(hidden, w_shard.T, inv_temp.reshape(halves, LANES), target_id.reshape(halves, LANES))
        shared = pl.pallas_call(
            functools.partial(exchange_kernel, n_vocab, n_inner),
            name='exchange',
            out_shape=[pltpu.VMEM(block, f32), pltpu.VMEM(small, f32), pltpu.VMEM(small, f32),
                       pltpu.VMEM((2, halves, SUB, LANES), f32), pltpu.VMEM((halves, LANES), f32)],
            in_specs=[vmem] * 6,
            out_specs=[vmem] * 5,
            scratch_shapes=[pltpu.VMEM(block, f32), pltpu.VMEM((peers, SUB, LANES), f32),
                            pltpu.SemaphoreType.DMA, pltpu.SemaphoreType.DMA],
            compiler_params=pltpu.CompilerParams(collective_id=0, has_side_effects=True, vmem_limit_bytes=4 * 2**20),
        )(*state)
        table, target = pl.pallas_call(
            finish_kernel,
            name='finish',
            out_shape=[pltpu.HBM(packed, f32), pltpu.HBM((halves, LANES), f32)],
            in_specs=[vmem] * 6,
            out_specs=[pl.BlockSpec(memory_space=pltpu.HBM)] * 2,
            scratch_shapes=[pltpu.VMEM(packed, f32), pltpu.SemaphoreType.DMA((2,))],
            compiler_params=pltpu.CompilerParams(vmem_limit_bytes=20 * 2**20),
        )(c, *shared)
        return table.transpose(0, 2, 1, 3).reshape(width, rows).T, target.reshape(rows)

    return jax.shard_map(local_step, mesh=mesh, in_specs=(P('dp', None), P(None, VOCAB_AXES), P('dp'), P('dp')), out_specs=(P('dp', VOCAB_AXES), P('dp')), check_vma=False)
```

```python
import functools

import jax
import jax.numpy as jnp
from jax import lax
from jax.experimental import pallas as pl
from jax.experimental.pallas import tpu as pltpu
from jax.sharding import PartitionSpec as P

VOCAB_AXES = ('vocab', 'inner')
MESH = pl.DeviceIdType.MESH
LANES = 128
SUB = 8
BODY = 800
WIDE = 256
BLOCKS = 25
EARLY_K = 5


def hint(x, k):
    return x if isinstance(x, int) else pl.multiple_of(x, k)


def above(x, sub):
    total = x
    for d in (1, 2, 4):
        total = total + jnp.where(sub >= d, pltpu.roll(total, d, 0), 0.0)
    return total - x, jnp.broadcast_to(total[SUB - 1:SUB, :], (SUB, LANES))


def weigh(start, tops, tgt_v, zbuf, ebuf, c_ref, first):
    halves = len(tops)
    run = BODY // SUB
    sub = lax.broadcasted_iota(jnp.int32, (SUB, LANES), 0)
    out = []
    for i in range(halves):
        top = jnp.broadcast_to(jnp.max(tops[i], axis=0, keepdims=True), (SUB, LANES))
        sums = [jnp.zeros((SUB, LANES), jnp.float32)] * 4
        for j in range(run):
            e = jnp.exp(zbuf[i, pl.ds(j, SUB, stride=run), :] - top)
            ebuf[i, pl.ds(j * SUB, SUB), :] = e
            sums[j % 4] = sums[j % 4] + e
        running, total = above((sums[0] + sums[1]) + (sums[2] + sums[3]), sub)
        goal = tgt_v[pl.ds(i, 1), :] - start
        upto = jnp.where((goal >= BODY) & (sub == 0), total, 0.0)
        goal = goal - sub * run
        for j in range(run):
            running = running + ebuf[i, pl.ds(j * SUB, SUB), :]
            c_ref[i, pl.ds(first + j, SUB, stride=run), :] = running
            upto = jnp.where(goal == j, running, upto)
        out.append((top, total, upto))
    return out


def stream_kernel(h_hbm, w_hbm, inv_hbm, tgt_hbm,
                  c_ref, zbuf, top_ref, m_tile, s_tile, t_tile, tgt_v,
                  h_v, wbuf, inv_v, ebuf, in_sem, w_sem):
    rows, depth = h_v.shape
    width = w_hbm.shape[0]
    halves = rows // LANES
    count = width // BODY
    part = BODY // 2
    run = BODY // SUB
    me = lax.axis_index('vocab') * lax.axis_size('inner') + lax.axis_index('inner')
    sub = lax.broadcasted_iota(jnp.int32, (SUB, LANES), 0)

    def w_copy(t, piece):
        here = pl.ds(hint(t * BODY, 16), BODY)
        cut = EARLY_K * WIDE
        there = pl.ds(0, cut) if piece == 0 else pl.ds(cut, depth - cut)
        return pltpu.make_async_copy(w_hbm.at[here, there], wbuf.at[here, there], w_sem.at[t, piece])

    small = [pltpu.make_async_copy(h_hbm, h_v, in_sem.at[0]),
             pltpu.make_async_copy(inv_hbm, inv_v, in_sem.at[1]),
             pltpu.make_async_copy(tgt_hbm, tgt_v, in_sem.at[2])]
    for copy in small:
        copy.start()

    @pl.loop(0, count)
    def _(t):
        w_copy(t, 0).start()
        w_copy(t, 1).start()

    for copy in small:
        copy.wait()

    def multiply(*accs):
        accs = (accs[:2], accs[2:])

        def push(k):
            for q in range(2):
                pltpu.matmul_push_rhs(h_v[:, pl.ds(k * WIDE, WIDE)], 0, q, transpose=True)

        def drain(t, slot):
            tops = [None] * halves
            for q in range(2):
                z = pltpu.matmul_pop(accs[q][slot])
                for i in range(halves):
                    zi = z[:, i * LANES:(i + 1) * LANES] * inv_v[pl.ds(i, 1), :]
                    zbuf[i, pl.ds(q * part, part), :] = zi
                    top = jnp.max(zi.reshape(part // SUB, SUB, LANES), axis=0)
                    tops[i] = top if q == 0 else jnp.maximum(tops[i], top)
            return tops

        def step(t, slot, first=False, final=False):
            for k in range(depth // WIDE):
                if k in (0, EARLY_K):
                    w_copy(t, k // EARLY_K).wait()
                for q in range(2):
                    pltpu.matmul_acc_lhs(
                        accs[q][slot], wbuf[pl.ds(hint(t * BODY + q * part, 16), part), pl.ds(k * WIDE, WIDE)],
                        load_staged_rhs=0)
                if k < depth // WIDE - 1:
                    push(k + 1)
                elif not final:
                    push(0)
                if k == 1 and not first:
                    tops = drain(t - 1, 1 - slot)
                if k == EARLY_K and not first:
                    start = (t - 1) * BODY
                    for i, (m, s, u) in enumerate(weigh(me * width + start, tops, tgt_v, zbuf, ebuf, c_ref, start)):
                        m_tile[t - 1, i] = m
                        s_tile[t - 1, i] = s
                        t_tile[t - 1, i] = u

        for q in range(2):
            for slot in range(2):
                pltpu.matmul_pop(accs[q][slot])
        push(0)
        step(0, 0, first=True)
        step(1, 1)

        @pl.loop(1, count // 2 - 1)
        def _(p):
            step(2 * p, 0)
            step(2 * p + 1, 1)

        step(count - 2, 0)
        step(count - 1, 1, final=True)
        for i, top in enumerate(drain(count - 1, 1)):
            top_ref[i] = top

    pl.run_scoped(multiply, *[pltpu.ACC(q)((part, rows), jnp.float32) for q in (0, 0, 1, 1)])


def exchange_kernel(n_vocab, n_inner, zbuf, top_ref, m_tile, s_tile, t_tile, tgt_v,
                    c_last, scale_ref, start_ref, ends_ref, ct_ref, ebuf, stats, send_sem, recv_sem):
    peers = n_vocab * n_inner
    halves = ct_ref.shape[0]
    my_vocab, my_inner = lax.axis_index('vocab'), lax.axis_index('inner')
    me = my_vocab * n_inner + my_inner

    far = sorted(((dv, di) for dv in range(n_vocab) for di in range(n_inner) if dv or di),
                 key=lambda o: -(min(o[0], n_vocab - o[0]) / 2 + min(o[1], n_inner - o[1])))

    def peer(dv, di):
        return {'vocab': lax.rem(my_vocab + dv, n_vocab), 'inner': lax.rem(my_inner + di, n_inner)}

    barrier = pltpu.get_barrier_semaphore()
    for offset in far:
        pl.semaphore_signal(barrier, inc=1, device_id=peer(*offset), device_id_type=MESH)

    count = m_tile.shape[0] + 1
    last = (count - 1) * BODY
    final = weigh(me * (count * BODY) + last, [top_ref[i] for i in range(halves)], tgt_v, zbuf, ebuf, c_last, 0)
    sub = lax.broadcasted_iota(jnp.int32, (SUB, LANES), 0)
    mix = jnp.zeros((SUB, LANES), jnp.float32)
    for i in range(halves):
        known = [(m_tile[t, i], s_tile[t, i], t_tile[t, i]) for t in range(count - 1)] + [final[i]]
        m = functools.reduce(jnp.maximum, [k[0] for k in known])
        s = jnp.zeros((SUB, LANES), jnp.float32)
        u = jnp.zeros((SUB, LANES), jnp.float32)
        for t in range(count):
            f = jnp.exp(known[t][0] - m)
            scale_ref[t, i] = f
            start_ref[t, i] = s
            s = s + known[t][1] * f
            u = u + known[t][2] * f
        mix = jnp.where((sub == 4 * i) | (sub == 4 * i + 1), m, mix)
        mix = jnp.where(sub == 4 * i + 2, s, mix)
        mix = jnp.where(sub == 4 * i + 3, jnp.sum(u, axis=0, keepdims=True), mix)
    stats[me] = mix
    pl.semaphore_wait(barrier, peers - 1)
    for offset in far:
        pltpu.make_async_remote_copy(
            src_ref=stats.at[me], dst_ref=stats.at[me], send_sem=send_sem, recv_sem=recv_sem,
            device_id=peer(*offset), device_id_type=MESH).start()

    everyone = stats.at[pl.ds(0, peers - 1)]
    done = pltpu.make_async_remote_copy(
        src_ref=everyone, dst_ref=everyone, send_sem=send_sem, recv_sem=recv_sem,
        device_id=peer(0, 0), device_id_type=MESH)
    done.wait_recv()

    peak = stats[0]
    for p in range(1, peers):
        peak = jnp.maximum(peak, stats[p])
    whole = jnp.zeros((SUB, LANES), jnp.float32)
    before = jnp.zeros((SUB, LANES), jnp.float32)
    for p in range(peers):
        mass = pltpu.roll(jnp.exp(stats[p] - peak), 2, 0) * stats[p]
        whole = whole + mass
        before = before + jnp.where(p < me, mass, 0.0)
    factor = pltpu.roll(jnp.exp(stats[me] - peak), 2, 0) / whole
    offset = before / whole
    reached = whole / pltpu.roll(whole, 1, 0)
    for i in range(halves):
        ct_ref[pl.ds(i, 1), :] = reached[4 * i + 3:4 * i + 4, :]
        ends_ref[0, i] = jnp.broadcast_to(factor[4 * i + 2:4 * i + 3, :], (SUB, LANES))
        ends_ref[1, i] = jnp.broadcast_to(offset[4 * i + 2:4 * i + 3, :], (SUB, LANES))
    done.wait_send()


def finish_kernel(c_ref, c_last, scale_ref, start_ref, ends_ref, ct_ref, out_hbm, ct_out, stage, sem):
    halves = c_ref.shape[0]
    parts = BODY // SUB // BLOCKS
    early = c_ref.shape[1] // SUB // BLOCKS
    target = pltpu.make_async_copy(ct_ref, ct_out, sem.at[1])
    target.start()

    def emit(b, source, origin):
        t = b // parts
        scale = [scale_ref[t, i] * ends_ref[0, i] for i in range(halves)]
        offset = [start_ref[t, i] * ends_ref[0, i] + ends_ref[1, i] for i in range(halves)]
        first = b * BLOCKS
        for k in range(BLOCKS):
            for i in range(halves):
                v = source[i, pl.ds(hint((first - origin + k) * SUB, SUB), SUB), :]
                stage[first + k, i] = v * scale[i] + offset[i]
        here = pl.ds(first, BLOCKS)
        pltpu.make_async_copy(stage.at[here], out_hbm.at[here], sem.at[0]).start()

    @pl.loop(0, early)
    def _(b):
        emit(b, c_ref, 0)

    @pl.loop(early, early + parts)
    def _(b):
        emit(b, c_last, early * BLOCKS)

    pltpu.make_async_copy(stage, out_hbm, sem.at[0]).wait()
    target.wait()


def solution(mesh):
    n_vocab, n_inner = mesh.shape['vocab'], mesh.shape['inner']
    peers = n_vocab * n_inner
    f32, bf16 = jnp.float32, jnp.bfloat16
    hbm = pl.BlockSpec(memory_space=pl.ANY)
    vmem = pl.BlockSpec(memory_space=pltpu.VMEM)

    def local_step(hidden, w_shard, inv_temp, target_id):
        rows, depth = hidden.shape
        width = w_shard.shape[1]
        halves = rows // LANES
        tiles = width // BODY
        small, early = (tiles, halves, SUB, LANES), (tiles - 1, halves, SUB, LANES)
        block = (halves, BODY, LANES)
        packed = (width // SUB, halves, SUB, LANES)
        c, *state = pl.pallas_call(
            stream_kernel,
            name='stream',
            out_shape=[pltpu.VMEM((halves, width - BODY, LANES), f32), pltpu.VMEM(block, f32),
                       pltpu.VMEM((halves, SUB, LANES), f32), pltpu.VMEM(early, f32), pltpu.VMEM(early, f32),
                       pltpu.VMEM(early, f32), pltpu.VMEM((halves, LANES), jnp.int32)],
            in_specs=[hbm] * 4,
            out_specs=[vmem] * 7,
            scratch_shapes=[
                pltpu.VMEM((rows, depth), bf16),
                pltpu.VMEM((width, depth), bf16),
                pltpu.VMEM((halves, LANES), f32),
                pltpu.VMEM(block, f32),
                pltpu.SemaphoreType.DMA((3,)),
                pltpu.SemaphoreType.DMA((tiles, 2)),
            ],
            compiler_params=pltpu.CompilerParams(vmem_limit_bytes=50 * 2**20),
        )(hidden, w_shard.T, inv_temp.reshape(halves, LANES), target_id.reshape(halves, LANES))
        shared = pl.pallas_call(
            functools.partial(exchange_kernel, n_vocab, n_inner),
            name='exchange',
            out_shape=[pltpu.VMEM(block, f32), pltpu.VMEM(small, f32), pltpu.VMEM(small, f32),
                       pltpu.VMEM((2, halves, SUB, LANES), f32), pltpu.VMEM((halves, LANES), f32)],
            in_specs=[vmem] * 6,
            out_specs=[vmem] * 5,
            scratch_shapes=[pltpu.VMEM(block, f32), pltpu.VMEM((peers, SUB, LANES), f32),
                            pltpu.SemaphoreType.DMA, pltpu.SemaphoreType.DMA],
            compiler_params=pltpu.CompilerParams(collective_id=0, has_side_effects=True, vmem_limit_bytes=4 * 2**20),
        )(*state)
        table, target = pl.pallas_call(
            finish_kernel,
            name='finish',
            out_shape=[pltpu.HBM(packed, f32), pltpu.HBM((halves, LANES), f32)],
            in_specs=[vmem] * 6,
            out_specs=[pl.BlockSpec(memory_space=pltpu.HBM)] * 2,
            scratch_shapes=[pltpu.VMEM(packed, f32), pltpu.SemaphoreType.DMA((2,))],
            compiler_params=pltpu.CompilerParams(vmem_limit_bytes=20 * 2**20),
        )(c, *shared)
        return table.transpose(0, 2, 1, 3).reshape(width, rows).T, target.reshape(rows)

    return jax.shard_map(local_step, mesh=mesh, in_specs=(P('dp', None), P(None, VOCAB_AXES), P('dp'), P('dp')), out_specs=(P('dp', VOCAB_AXES), P('dp')), check_vma=False)
```
